32 devices in a mesh: bank: 4 (over z), lane: 4 (over y, core), site: 2 (over x).
Axes of the slice: x: 2, y: 2, z: 4, core: 2. Of those that a mesh axis runs over, the one named last changes fastest.
Arguments:
- wave_parts: float32 [4, 64, 128, 128], P('site', ('bank', 'lane')), parts along dimension 0, may hold values from -6 to 6
- level_table: float32 [128, 128, 128], P(('site', 'bank', 'lane')), parts along dimension 0, may hold values from -2 to 2
- phase_angles: float32 [4, 128], P('site'), parts along dimension 0, may hold values from 0.3 to 1.2
- mix_angles: float32 [4, 4], P('site'), parts along dimension 0, may hold values from 0.3 to 1.2
Outputs:
- final_parts: float32 [4, 64, 128, 128], P('site', ('bank', 'lane')), parts along dimension 0
The draws below stay inside these ranges and needn't reach their ends.
There are 2 independent parts, one for each index of `site`. The reference program is written for one: setup_inputs(seed, part) draws one part's arguments, and reference() takes and returns one part's arrays. A program takes and returns all parts, laid end to end along the dimension named above; each array names one. Nothing has to cross between parts.
All inputs are finite; a program needn't handle non-finite values.
Results may differ from the reference program's by a relative error of at most 0.0003.
Values sent between devices are 32-bit elements; how exact they have to be, the bound alone decides.
A program may use at most 64 MiB of HBM per device.

```python
import jax
import jax.numpy as jnp
from jax import lax

BLOCKS_DEV = 4
ROWS = 128
LANES = 128
BLOCKS = 64
LAYERS = 2
N_BANK = 4
N_LANE = 4


def level_of(key, extent, pieces, low, largest):
    gain, own = 1.0, jax.random.fold_in(key, 6)
    for axis_at, shards_of in pieces:
        heights = jnp.exp(jax.random.uniform(jax.random.fold_in(own, axis_at), (shards_of,), jnp.float32, low / len(pieces), largest / len(pieces)))
        gain = gain * jnp.repeat(heights, extent[axis_at] // shards_of).reshape([-1 if axis == axis_at else 1 for axis in range(len(extent))])
    return gain


def noise(stream_key, dims, deviation, reach, pieces=(), kind=jnp.bfloat16):
    array = jax.random.normal(stream_key, dims, jnp.float32) * deviation
    if len(pieces) > 0:
        array = level_of(stream_key, dims, pieces, -0.22, 0.18) * array
    return jnp.clip(array, min=-reach, max=reach).astype(kind)


def setup_inputs(seed: int = 0, part: int = 0) -> dict:
    arg_keys = jax.random.split(jax.random.key(seed), 5)
    own_keys = jax.random.split(jax.random.fold_in(arg_keys[4], part), 5)
    wave_parts = noise(own_keys[0], (2, BLOCKS, ROWS, LANES), 1.0, 6.0, ((1, 16),), jnp.float32)
    level_table = jnp.clip(jax.random.uniform(own_keys[1], (BLOCKS, ROWS, LANES), jnp.float32, -2.0, 2.0) * level_of(own_keys[1], (BLOCKS, ROWS, LANES), ((0, 16),), -0.4, 0.0), -2.0, 2.0)
    phase_angles = jnp.clip(jax.random.uniform(own_keys[2], (LAYERS, LANES), jnp.float32, 0.3, 1.2), 0.3, 1.2)
    mix_angles = jnp.clip(jax.random.uniform(own_keys[3], (LAYERS, 4), jnp.float32, 0.3, 1.2), 0.3, 1.2)
    return dict(wave_parts=wave_parts, level_table=level_table, phase_angles=phase_angles, mix_angles=mix_angles)


def count_bits(values, count):
    places = jnp.arange(count.bit_length() - 1, dtype=jnp.int32)
    return jnp.sum((values[..., None] >> places) & 1, axis=-1)


def plane_table(count, angle):
    rank = jnp.arange(count, dtype=jnp.int32)
    apart = count_bits(rank[:, None] ^ rank[None, :], count)
    minus = count_bits(rank[:, None] & (rank[:, None] ^ rank[None, :]), count)
    bits = count.bit_length() - 1
    size = jnp.cos(angle) ** (bits - apart).astype(jnp.float32) * jnp.sin(angle) ** apart.astype(jnp.float32)
    return size * jnp.where(minus % 2 == 1, -1.0, 1.0).astype(jnp.float32)


def apply_along(values, dim, angle):
    real_part = plane_table(values.shape[dim], angle)
    def times(table):
        moved = jnp.tensordot(values, table, axes=([dim], [0]), precision=lax.Precision.HIGHEST)
        return jnp.moveaxis(moved, -1, dim)
    return times(real_part)


def turn_phase(values, levels, angle):
    turn = angle * levels
    return jnp.stack([values[0] * jnp.cos(turn) + values[1] * jnp.sin(turn), values[1] * jnp.cos(turn) - values[0] * jnp.sin(turn)])


def reference(wave_parts, level_table, phase_angles, mix_angles):
    values = wave_parts
    for layer in range(LAYERS):
        values = turn_phase(values, level_table, phase_angles[layer])
        values = apply_along(values, 3, mix_angles[layer, 0])
        values = apply_along(values, 2, mix_angles[layer, 1])
        parts = values.reshape(2, N_BANK, N_LANE, BLOCKS_DEV, ROWS, LANES)
        parts = apply_along(parts, 1, mix_angles[layer, 2])
        parts = apply_along(parts, 2, mix_angles[layer, 3])
        parts = apply_along(parts, 3, mix_angles[layer, 2])
        values = parts.reshape(values.shape)
    return values
```

```python
import functools

import jax
import jax.numpy as jnp
from jax import lax
from jax.experimental import pallas as pl
from jax.experimental.pallas import tpu as pltpu
from jax.sharding import PartitionSpec as P

SUB = 8
MESH = pl.DeviceIdType.MESH


def sin_cos(turn):
    h = 0.5 * turn
    q = h * h
    s = -1.0 / 39916800 + q * (1.0 / 6227020800)
    for term in (1.0 / 362880, -1.0 / 5040, 1.0 / 120, -1.0 / 6, 1.0):
        s = term + q * s
    s = h * s
    c = -1.0 / 3628800 + q * (1.0 / 479001600)
    for term in (1.0 / 40320, -1.0 / 720, 1.0 / 24, -0.5, 1.0):
        c = term + q * c
    return 2.0 * s * c, 1.0 - 2.0 * s * s


def rotate_bits(x, count, sc):
    s, c = sc
    shape = x.shape
    step = 1
    while step < count:
        y = x.reshape(count // (2 * step), 2, step, *shape[1:])
        u, v = y[:, 0], y[:, 1]
        x = jnp.stack([c * u - s * v, c * v + s * u], axis=1).reshape(shape)
        step *= 2
    return x


def rotate_sublanes(x, sc):
    s, c = sc
    place = lax.broadcasted_iota(jnp.int32, s.shape, 0)
    step = 1
    while step < SUB:
        upper = (place // step) % 2 == 1
        down = pltpu.roll(x, step, 1)
        if 2 * step == SUB:
            x = c * x + jnp.where(upper, s, -s) * down
        else:
            up = pltpu.roll(x, SUB - step, 1)
            x = c * x + jnp.where(upper, s, -s) * jnp.where(upper, down, up)
        step *= 2
    return x


def lane_table(sc, lanes):
    s = jnp.broadcast_to(sc[0][0:1], (lanes, lanes))
    c = jnp.broadcast_to(sc[1][0:1], (lanes, lanes))
    i = lax.broadcasted_iota(jnp.int32, (lanes, lanes), 0)
    j = lax.broadcasted_iota(jnp.int32, (lanes, lanes), 1)
    table = jnp.ones((lanes, lanes), jnp.float32)
    step = 1
    while step < lanes:
        a, b = (i // step) % 2, (j // step) % 2
        table = table * jnp.where(a == b, c, jnp.where(a > b, -s, s))
        step *= 2
    high = table.astype(jnp.bfloat16)
    low = (table - high.astype(jnp.float32)).astype(jnp.bfloat16)
    top = jnp.concatenate([high, low], axis=1)
    bottom = jnp.concatenate([high, jnp.zeros_like(low)], axis=1)
    return jnp.concatenate([top, bottom], axis=0)


def rotate_lanes(x, table):
    lanes = x.shape[1]
    high = x.astype(jnp.bfloat16)
    low = (x - high.astype(jnp.float32)).astype(jnp.bfloat16)
    out = jnp.dot(
        jnp.concatenate([high, low], axis=1), table, preferred_element_type=jnp.float32
    )
    return out[:, :lanes] + out[:, lanes:]


def kernel(
    n_bank, n_lane, chunks,
    wave_hbm, level_hbm, phase_ref, mix_ref, out_ref,
    wave, level, mixed, send, recv, level_recv, turned, back,
    in_sem, level_send_sem, level_recv_sem, send_sem, recv_sem, turn_sem, back_sem,
):
    n = n_bank * n_lane
    bank, lane = lax.axis_index("bank"), lax.axis_index("lane")
    me = bank * n_lane + lane
    _, blocks, rows, lanes = wave.shape
    tiles = rows // SUB
    units = blocks * tiles // n
    each = units // chunks

    peers = []
    order = [n_bank // 2] + [k for k in range(n_bank) if k != n_bank // 2]
    for kb in order:
        for kl in range(n_lane):
            if kb or kl:
                pb, pn = lax.rem(bank + kb, n_bank), lax.rem(lane + kl, n_lane)
                peers.append(({"bank": pb, "lane": pn}, pb * n_lane + pn))

    barrier = pltpu.get_barrier_semaphore()
    for device, _ in peers:
        pl.semaphore_signal(barrier, inc=1, device_id=device, device_id_type=MESH)
    load_wave = pltpu.make_async_copy(wave_hbm, wave, in_sem.at[0])
    load_level = pltpu.make_async_copy(level_hbm, level, in_sem.at[1])
    load_level.start()
    load_wave.start()

    sc = [[sin_cos(jnp.full((SUB, lanes), mix_ref[y, g], jnp.float32)) for g in range(4)] for y in range(2)]
    tables = [lane_table(sc[y][0], lanes) for y in range(2)]

    load_level.wait()
    load_wave.wait()
    for block in range(blocks):
        here = level[block * tiles : (block + 1) * tiles].reshape(rows, lanes)
        s, c = sin_cos(phase_ref[0:1, :] * here)
        real, imag = wave[0, block], wave[1, block]
        x = jnp.concatenate([real * c + imag * s, imag * c - real * s], axis=0)
        x = rotate_lanes(x, tables[0])
        x = rotate_sublanes(x.reshape(2 * tiles, SUB, lanes), sc[0][1])
        x = x.reshape(2, tiles, SUB, lanes)
        for part in range(2):
            mixed[part, block] = rotate_bits(x[part], tiles, sc[0][1])

    pl.semaphore_wait(barrier, n - 1)
    for device, there in peers:
        pltpu.make_async_remote_copy(
            src_ref=level_units(level, there, units),
            dst_ref=level_recv.at[me],
            send_sem=level_send_sem,
            recv_sem=level_recv_sem,
            device_id=device,
            device_id_type=MESH,
        ).start()
    level_recv[me] = level_units(level, me, units)[...]

    for part in range(2):
        x = rotate_bits(mixed[part], blocks, sc[0][2])
        x = x.reshape(n, chunks, each, SUB, lanes)
        for k in range(chunks):
            send[k, :, part] = x[:, k]
    for k in range(chunks):
        for device, there in peers:
            pltpu.make_async_remote_copy(
                src_ref=send.at[k, there],
                dst_ref=recv.at[k, me],
                send_sem=send_sem.at[k],
                recv_sem=recv_sem.at[k],
                device_id=device,
                device_id_type=MESH,
            ).start()
        recv[k, me] = send[k, me]

    def wait_all(buffer, sem):
        whole = buffer.at[pl.ds(0, n - 1)]
        pltpu.make_async_copy(whole, whole, sem).wait()

    wait_all(level_recv, level_recv_sem)
    for k in range(chunks):
        wait_all(recv.at[k], recv_sem.at[k])
        x = recv[k].reshape(n_bank, n_lane, 2, each, SUB, lanes)
        x = rotate_bits(x, n_bank, sc[0][2])
        x = jnp.stack([rotate_bits(x[b], n_lane, sc[0][3]) for b in range(n_bank)])
        x = x.reshape(n, 2, each, SUB, lanes)
        s, c = sin_cos(phase_ref[1:2, :] * level_recv[:, k * each : (k + 1) * each])
        real, imag = x[:, 0], x[:, 1]
        x = jnp.stack([real * c + imag * s, imag * c - real * s], axis=1)
        x = rotate_lanes(x.reshape(n * 2 * each * SUB, lanes), tables[1])
        x = rotate_sublanes(x.reshape(n * 2 * each, SUB, lanes), sc[1][1])
        x = x.reshape(n_bank, n_lane, 2, each, SUB, lanes)
        x = rotate_bits(x, n_bank, sc[1][2])
        x = jnp.stack([rotate_bits(x[b], n_lane, sc[1][3]) for b in range(n_bank)])
        turned[k] = x.reshape(n, 2, each, SUB, lanes)
        for device, there in peers:
            pltpu.make_async_remote_copy(
                src_ref=turned.at[k, there],
                dst_ref=back.at[k, me],
                send_sem=turn_sem.at[k],
                recv_sem=back_sem.at[k],
                device_id=device,
                device_id_type=MESH,
            ).start()
        back[k, me] = turned[k, me]

    for k in range(chunks):
        wait_all(back.at[k], back_sem.at[k])
    for part in range(2):
        x = jnp.stack([back[k, :, part] for k in range(chunks)], axis=1)
        x = x.reshape(blocks, tiles, SUB, lanes)
        x = rotate_bits(x, blocks, sc[1][2])
        for block in range(blocks):
            out_ref[part, block] = rotate_bits(x[block], tiles, sc[1][1]).reshape(rows, lanes)

    wait_all(level_recv, level_send_sem)
    for k in range(chunks):
        wait_all(recv.at[k], send_sem.at[k])
        wait_all(back.at[k], turn_sem.at[k])


def level_units(level, there, units):
    return level.at[pl.ds(there * units, units)]


def local(n_bank, n_lane, wave_parts, level_table, phase_angles, mix_angles):
    parts, blocks, rows, lanes = wave_parts.shape
    n = n_bank * n_lane
    tiles = rows // SUB
    units = blocks * tiles // n
    chunks = min(4, units)
    each = units // chunks
    exchange = pltpu.VMEM((chunks, n, 2, each, SUB, lanes), jnp.float32)
    dma = pltpu.SemaphoreType.DMA
    return pl.pallas_call(
        functools.partial(kernel, n_bank, n_lane, chunks),
        out_shape=jax.ShapeDtypeStruct(wave_parts.shape, jnp.float32),
        in_specs=[
            pl.BlockSpec(memory_space=pl.ANY),
            pl.BlockSpec(memory_space=pl.ANY),
            pl.BlockSpec(memory_space=pltpu.VMEM),
            pl.BlockSpec(memory_space=pltpu.SMEM),
        ],
        out_specs=pl.BlockSpec(memory_space=pltpu.VMEM),
        scratch_shapes=[
            pltpu.VMEM(wave_parts.shape, jnp.float32),
            pltpu.VMEM((blocks * tiles, SUB, lanes), jnp.float32),
            pltpu.VMEM((2, blocks, tiles, SUB, lanes), jnp.float32),
            exchange,
            exchange,
            pltpu.VMEM((n, units, SUB, lanes), jnp.float32),
            exchange,
            exchange,
            dma((2,)),
            dma,
            dma,
            dma((chunks,)),
            dma((chunks,)),
            dma((chunks,)),
            dma((chunks,)),
        ],
        compiler_params=pltpu.CompilerParams(
            collective_id=0, has_side_effects=True, vmem_limit_bytes=48 * 1024 * 1024
        ),
    )(wave_parts, level_table.reshape(blocks * tiles, SUB, lanes), phase_angles, mix_angles)


def solution(mesh):
    placed = (
        P("site", ("bank", "lane"), None, None),
        P(("site", "bank", "lane"), None, None),
        P("site", None),
        P("site", None),
    )
    return jax.shard_map(
        functools.partial(local, mesh.shape["bank"], mesh.shape["lane"]),
        mesh=mesh,
        in_specs=placed,
        out_specs=P("site", ("bank", "lane"), None, None),
        check_vma=False,
    )
```

```python
import functools

import jax
import jax.numpy as jnp
from jax import lax
from jax.experimental import pallas as pl
from jax.experimental.pallas import tpu as pltpu
from jax.sharding import PartitionSpec as P

SUB = 8
MESH = pl.DeviceIdType.MESH


def sin_cos(turn):
    h = 0.5 * turn
    q = h * h
    s = -1.0 / 39916800 + q * (1.0 / 6227020800)
    for term in (1.0 / 362880, -1.0 / 5040, 1.0 / 120, -1.0 / 6, 1.0):
        s = term + q * s
    s = h * s
    c = -1.0 / 3628800 + q * (1.0 / 479001600)
    for term in (1.0 / 40320, -1.0 / 720, 1.0 / 24, -0.5, 1.0):
        c = term + q * c
    return 2.0 * s * c, 1.0 - 2.0 * s * s


def rotate_bits(x, count, sc):
    s, c = sc
    shape = x.shape
    step = 1
    while step < count:
        y = x.reshape(count // (2 * step), 2, step, *shape[1:])
        u, v = y[:, 0], y[:, 1]
        x = jnp.stack([c * u - s * v, c * v + s * u], axis=1).reshape(shape)
        step *= 2
    return x


def rotate_list(items, sc):
    s, c = sc
    step = 1
    while step < len(items):
        items = [
            c * x - s * items[i + step] if (i // step) % 2 == 0 else c * x + s * items[i - step]
            for i, x in enumerate(items)
        ]
        step *= 2
    return items


def differ(index, apart, count):
    out, bit = 0, 1
    while bit < count:
        out = out + lax.rem(index // bit + (apart // bit) % 2, 2) * bit
        bit *= 2
    return out


def rotate_sublanes(x, sc):
    s, c = sc
    place = lax.broadcasted_iota(jnp.int32, s.shape, 0)
    step = 1
    while step < SUB:
        upper = (place // step) % 2 == 1
        down = pltpu.roll(x, step, 1)
        if 2 * step == SUB:
            x = c * x + jnp.where(upper, s, -s) * down
        else:
            up = pltpu.roll(x, SUB - step, 1)
            x = c * x + jnp.where(upper, s, -s) * jnp.where(upper, down, up)
        step *= 2
    return x


def lane_table(sc, lanes):
    s = jnp.broadcast_to(sc[0][0:1], (lanes, lanes))
    c = jnp.broadcast_to(sc[1][0:1], (lanes, lanes))
    i = lax.broadcasted_iota(jnp.int32, (lanes, lanes), 0)
    j = lax.broadcasted_iota(jnp.int32, (lanes, lanes), 1)
    table = jnp.ones((lanes, lanes), jnp.float32)
    step = 1
    while step < lanes:
        a, b = (i // step) % 2, (j // step) % 2
        table = table * jnp.where(a == b, c, jnp.where(a > b, -s, s))
        step *= 2
    high = table.astype(jnp.bfloat16)
    low = (table - high.astype(jnp.float32)).astype(jnp.bfloat16)
    top = jnp.concatenate([high, low], axis=1)
    bottom = jnp.concatenate([high, jnp.zeros_like(low)], axis=1)
    return jnp.concatenate([top, bottom], axis=0)


def rotate_lanes(x, table):
    lanes = x.shape[1]
    high = x.astype(jnp.bfloat16)
    low = (x - high.astype(jnp.float32)).astype(jnp.bfloat16)
    out = jnp.dot(
        jnp.concatenate([high, low], axis=1), table, preferred_element_type=jnp.float32
    )
    return out[:, :lanes] + out[:, lanes:]


def kernel(
    n_bank, n_lane, chunks,
    wave_hbm, level_hbm, phase_hbm, mix_hbm, out_ref,
    wave, level, phase_ref, mix_ref, mixed, send, recv, level_recv, turned, back, last,
    in_sem, level_send_sem, level_recv_sem, send_sem, recv_sem, turn_sem, back_sem,
):
    n = n_bank * n_lane
    bank, lane = lax.axis_index("bank"), lax.axis_index("lane")
    me = bank * n_lane + lane
    _, blocks, rows, lanes = wave.shape
    tiles = rows // SUB
    units = blocks * tiles // n
    each = units // chunks

    peers = []
    for kb in range(n_bank - 1, -1, -1):
        for kl in range(n_lane - 1, -1, -1):
            if kb or kl:
                pb, pn = differ(bank, kb, n_bank), differ(lane, kl, n_lane)
                peers.append(({"bank": pb, "lane": pn}, pb * n_lane + pn))

    barrier = pltpu.get_barrier_semaphore()
    for device, _ in peers:
        pl.semaphore_signal(barrier, inc=1, device_id=device, device_id_type=MESH)
    loads = [
        pltpu.make_async_copy(there, here, in_sem.at[i])
        for i, (there, here) in enumerate(
            [(mix_hbm, mix_ref), (level_hbm, level), (phase_hbm, phase_ref), (wave_hbm, wave)]
        )
    ]
    for load in loads:
        load.start()

    loads[0].wait()
    sc = [[sin_cos(jnp.full((SUB, lanes), mix_ref[y, g], jnp.float32)) for g in range(4)] for y in range(2)]
    tables = [lane_table(sc[y][0], lanes) for y in range(2)]

    for load in loads[1:]:
        load.wait()
    pl.semaphore_wait(barrier, n - 1)
    for device, there in peers:
        pltpu.make_async_remote_copy(
            src_ref=level_units(level, there, units),
            dst_ref=level_recv.at[me],
            send_sem=level_send_sem,
            recv_sem=level_recv_sem,
            device_id=device,
            device_id_type=MESH,
        ).start()
    level_recv[me] = level_units(level, me, units)[...]

    for block in range(blocks):
        here = level[block * tiles : (block + 1) * tiles].reshape(rows, lanes)
        s, c = sin_cos(phase_ref[0:1, :] * here)
        real, imag = wave[0, block], wave[1, block]
        x = jnp.concatenate([real * c + imag * s, imag * c - real * s], axis=0)
        x = rotate_lanes(x, tables[0])
        x = rotate_sublanes(x.reshape(2 * tiles, SUB, lanes), sc[0][1])
        x = x.reshape(2, tiles, SUB, lanes)
        for part in range(2):
            mixed[part, block] = rotate_bits(x[part], tiles, sc[0][1])

    for part in range(2):
        x = rotate_bits(mixed[part], blocks, sc[0][2])
        x = x.reshape(n, chunks, each, SUB, lanes)
        for k in range(chunks):
            send[k, :, part] = x[:, k]
    for k in range(chunks):
        for device, there in peers:
            pltpu.make_async_remote_copy(
                src_ref=send.at[k, there],
                dst_ref=recv.at[k, me],
                send_sem=send_sem.at[k],
                recv_sem=recv_sem.at[k],
                device_id=device,
                device_id_type=MESH,
            ).start()
        recv[k, me] = send[k, me]

    def wait_all(buffer, sem):
        whole = buffer.at[pl.ds(0, n - 1)]
        pltpu.make_async_copy(whole, whole, sem).wait()

    wait_all(level_recv, level_recv_sem)
    for k in range(chunks):
        wait_all(recv.at[k], recv_sem.at[k])
        x = recv[k].reshape(n_bank, n_lane, 2, each, SUB, lanes)
        x = rotate_bits(x, n_bank, sc[0][2])
        x = jnp.stack([rotate_bits(x[b], n_lane, sc[0][3]) for b in range(n_bank)])
        x = x.reshape(n, 2, each, SUB, lanes)
        s, c = sin_cos(phase_ref[1:2, :] * level_recv[:, k * each : (k + 1) * each])
        real, imag = x[:, 0], x[:, 1]
        x = jnp.stack([real * c + imag * s, imag * c - real * s], axis=1)
        x = rotate_lanes(x.reshape(n * 2 * each * SUB, lanes), tables[1])
        x = rotate_sublanes(x.reshape(n * 2 * each, SUB, lanes), sc[1][1])
        x = x.reshape(n_bank, n_lane, 2, each, SUB, lanes)
        x = rotate_bits(x, n_bank, sc[1][2])
        x = jnp.stack([rotate_bits(x[b], n_lane, sc[1][3]) for b in range(n_bank)])
        turned[k] = x.reshape(n, 2, each, SUB, lanes)
        for device, there in peers:
            pltpu.make_async_remote_copy(
                src_ref=turned.at[k, there],
                dst_ref=back.at[k, me],
                send_sem=turn_sem.at[k],
                recv_sem=back_sem.at[k],
                device_id=device,
                device_id_type=MESH,
            ).start()
        back[k, me] = turned[k, me]

    high = tiles // units
    for k in range(chunks):
        wait_all(back.at[k], back_sem.at[k])
        x = back[k].reshape(blocks, high, 2, each, SUB, lanes)
        x = rotate_bits(x, blocks, sc[1][2])
        x = jnp.stack([rotate_bits(x[b], high, sc[1][1]) for b in range(blocks)])
        last[k] = x.reshape(n, 2, each, SUB, lanes)
    for part in range(2):
        for block in range(blocks):
            these = pl.ds(block * high, high)
            items = [last[u // each, these, part, u % each] for u in range(units)]
            x = jnp.stack(rotate_list(items, sc[1][1]), axis=1)
            out_ref[part, block] = x.reshape(rows, lanes)

    wait_all(level_recv, level_send_sem)
    for k in range(chunks):
        wait_all(recv.at[k], send_sem.at[k])
        wait_all(back.at[k], turn_sem.at[k])


def level_units(level, there, units):
    return level.at[pl.ds(there * units, units)]


def local(n_bank, n_lane, wave_parts, level_table, phase_angles, mix_angles):
    parts, blocks, rows, lanes = wave_parts.shape
    n = n_bank * n_lane
    tiles = rows // SUB
    units = blocks * tiles // n
    chunks = min(4, units)
    each = units // chunks
    exchange = pltpu.VMEM((chunks, n, 2, each, SUB, lanes), jnp.float32)
    dma = pltpu.SemaphoreType.DMA
    return pl.pallas_call(
        functools.partial(kernel, n_bank, n_lane, chunks),
        out_shape=jax.ShapeDtypeStruct(wave_parts.shape, jnp.float32),
        in_specs=[
            pl.BlockSpec(memory_space=pltpu.HBM),
            pl.BlockSpec(memory_space=pltpu.HBM),
            pl.BlockSpec(memory_space=pltpu.HBM),
            pl.BlockSpec(memory_space=pltpu.HBM),
        ],
        out_specs=pl.BlockSpec(memory_space=pltpu.VMEM),
        scratch_shapes=[
            pltpu.VMEM(wave_parts.shape, jnp.float32),
            pltpu.VMEM((blocks * tiles, SUB, lanes), jnp.float32),
            pltpu.VMEM(phase_angles.shape, jnp.float32),
            pltpu.SMEM(mix_angles.shape, jnp.float32),
            pltpu.VMEM((2, blocks, tiles, SUB, lanes), jnp.float32),
            exchange,
            exchange,
            pltpu.VMEM((n, units, SUB, lanes), jnp.float32),
            exchange,
            exchange,
            exchange,
            dma((4,)),
            dma,
            dma,
            dma((chunks,)),
            dma((chunks,)),
            dma((chunks,)),
            dma((chunks,)),
        ],
        compiler_params=pltpu.CompilerParams(
            collective_id=0, has_side_effects=True, vmem_limit_bytes=67043328
        ),
    )(wave_parts, level_table.reshape(blocks * tiles, SUB, lanes), phase_angles, mix_angles)


def solution(mesh):
    placed = (
        P("site", ("bank", "lane"), None, None),
        P(("site", "bank", "lane"), None, None),
        P("site", None),
        P("site", None),
    )
    return jax.shard_map(
        functools.partial(local, mesh.shape["bank"], mesh.shape["lane"]),
        mesh=mesh,
        in_specs=placed,
        out_specs=P("site", ("bank", "lane"), None, None),
        check_vma=False,
    )
```

```python
import functools

import jax
import jax.numpy as jnp
from jax import lax
from jax.experimental import pallas as pl
from jax.experimental.pallas import tpu as pltpu
from jax.sharding import PartitionSpec as P

SUB = 8
MESH = pl.DeviceIdType.MESH


def sin_cos(turn):
    h = 0.5 * turn
    q = h * h
    s = -1.0 / 39916800 + q * (1.0 / 6227020800)
    for term in (1.0 / 362880, -1.0 / 5040, 1.0 / 120, -1.0 / 6, 1.0):
        s = term + q * s
    s = h * s
    c = -1.0 / 3628800 + q * (1.0 / 479001600)
    for term in (1.0 / 40320, -1.0 / 720, 1.0 / 24, -0.5, 1.0):
        c = term + q * c
    return 2.0 * s * c, 1.0 - 2.0 * s * s


def rotate_bits(x, count, sc):
    s, c = sc
    shape = x.shape
    step = 1
    while step < count:
        y = x.reshape(count // (2 * step), 2, step, *shape[1:])
        u, v = y[:, 0], y[:, 1]
        x = jnp.stack([c * u - s * v, c * v + s * u], axis=1).reshape(shape)
        step *= 2
    return x


def rotate_list(items, sc):
    s, c = sc
    step = 1
    while step < len(items):
        items = [
            c * x - s * items[i + step] if (i // step) % 2 == 0 else c * x + s * items[i - step]
            for i, x in enumerate(items)
        ]
        step *= 2
    return items


def differ(index, apart, count):
    out, bit = 0, 1
    while bit < count:
        out = out + lax.rem(index // bit + (apart // bit) % 2, 2) * bit
        bit *= 2
    return out


def rotate_sublanes(x, sc):
    s, c = sc
    place = lax.broadcasted_iota(jnp.int32, s.shape, 0)
    step = 1
    while step < SUB:
        upper = (place // step) % 2 == 1
        down = pltpu.roll(x, step, 1)
        if 2 * step == SUB:
            x = c * x + jnp.where(upper, s, -s) * down
        else:
            up = pltpu.roll(x, SUB - step, 1)
            x = c * x + jnp.where(upper, s, -s) * jnp.where(upper, down, up)
        step *= 2
    return x


def lane_table(sc, lanes):
    s = jnp.broadcast_to(sc[0][0:1], (lanes, lanes))
    c = jnp.broadcast_to(sc[1][0:1], (lanes, lanes))
    i = lax.broadcasted_iota(jnp.int32, (lanes, lanes), 0)
    j = lax.broadcasted_iota(jnp.int32, (lanes, lanes), 1)
    table = jnp.ones((lanes, lanes), jnp.float32)
    step = 1
    while step < lanes:
        a, b = (i // step) % 2, (j // step) % 2
        table = table * jnp.where(a == b, c, jnp.where(a > b, -s, s))
        step *= 2
    high = table.astype(jnp.bfloat16)
    low = (table - high.astype(jnp.float32)).astype(jnp.bfloat16)
    top = jnp.concatenate([high, low], axis=1)
    bottom = jnp.concatenate([high, jnp.zeros_like(low)], axis=1)
    return jnp.concatenate([top, bottom], axis=0)


def rotate_lanes(x, table):
    lanes = x.shape[1]
    high = x.astype(jnp.bfloat16)
    low = (x - high.astype(jnp.float32)).astype(jnp.bfloat16)
    out = jnp.dot(
        jnp.concatenate([high, low], axis=1), table, preferred_element_type=jnp.float32
    )
    return out[:, :lanes] + out[:, lanes:]


def kernel(
    n_bank, n_lane, chunks,
    wave_hbm, level_hbm, phase_hbm, mix_hbm, out_ref,
    wave, level, phase_ref, mix_ref, mixed, send, recv, level_recv, turned, back, last,
    in_sem, level_send_sem, level_recv_sem, send_sem, recv_sem, turn_sem, back_sem,
):
    n = n_bank * n_lane
    bank, lane = lax.axis_index("bank"), lax.axis_index("lane")
    me = bank * n_lane + lane
    _, blocks, rows, lanes = wave.shape
    tiles = rows // SUB
    units = blocks * tiles // n
    each = units // chunks

    peers = []
    for kb in range(n_bank - 1, -1, -1):
        for kl in range(n_lane - 1, -1, -1):
            if kb or kl:
                pb, pn = differ(bank, kb, n_bank), differ(lane, kl, n_lane)
                peers.append(({"bank": pb, "lane": pn}, pb * n_lane + pn))

    barrier = pltpu.get_barrier_semaphore()
    for device, _ in peers:
        pl.semaphore_signal(barrier, inc=1, device_id=device, device_id_type=MESH)
    loads = [
        pltpu.make_async_copy(there, here, in_sem.at[i])
        for i, (there, here) in enumerate(
            [(mix_hbm, mix_ref), (level_hbm, level), (phase_hbm, phase_ref), (wave_hbm, wave)]
        )
    ]
    for load in loads:
        load.start()

    loads[0].wait()
    sc = [[sin_cos(jnp.full((SUB, lanes), mix_ref[y, g], jnp.float32)) for g in range(4)] for y in range(2)]
    tables = [lane_table(sc[y][0], lanes) for y in range(2)]

    for load in loads[1:]:
        load.wait()
    pl.semaphore_wait(barrier, n - 1)
    for device, there in peers:
        pltpu.make_async_remote_copy(
            src_ref=level_units(level, there, units),
            dst_ref=level_recv.at[me],
            send_sem=level_send_sem,
            recv_sem=level_recv_sem,
            device_id=device,
            device_id_type=MESH,
        ).start()
    level_recv[me] = level_units(level, me, units)[...]

    for block in range(blocks):
        here = level[block * tiles : (block + 1) * tiles].reshape(rows, lanes)
        s, c = sin_cos(phase_ref[0:1, :] * here)
        real, imag = wave[0, block], wave[1, block]
        x = jnp.concatenate([real * c + imag * s, imag * c - real * s], axis=0)
        x = rotate_lanes(x, tables[0])
        x = rotate_sublanes(x.reshape(2 * tiles, SUB, lanes), sc[0][1])
        x = x.reshape(2, tiles, SUB, lanes)
        for part in range(2):
            mixed[part, block] = rotate_bits(x[part], tiles, sc[0][1])

    for part in range(2):
        x = rotate_bits(mixed[part], blocks, sc[0][2])
        x = x.reshape(n, chunks, each, SUB, lanes)
        for k in range(chunks):
            send[k, :, part] = x[:, k]
    for k in range(chunks):
        for device, there in peers:
            pltpu.make_async_remote_copy(
                src_ref=send.at[k, there],
                dst_ref=recv.at[k, me],
                send_sem=send_sem.at[k],
                recv_sem=recv_sem.at[k],
                device_id=device,
                device_id_type=MESH,
            ).start()
        recv[k, me] = send[k, me]

    def wait_all(buffer, sem):
        whole = buffer.at[pl.ds(0, n - 1)]
        pltpu.make_async_copy(whole, whole, sem).wait()

    wait_all(level_recv, level_recv_sem)
    for k in range(chunks):
        wait_all(recv.at[k], recv_sem.at[k])
        x = recv[k].reshape(n_bank, n_lane, 2, each, SUB, lanes)
        x = rotate_bits(x, n_bank, sc[0][2])
        x = jnp.stack([rotate_bits(x[b], n_lane, sc[0][3]) for b in range(n_bank)])
        x = x.reshape(n, 2, each, SUB, lanes)
        s, c = sin_cos(phase_ref[1:2, :] * level_recv[:, k * each : (k + 1) * each])
        real, imag = x[:, 0], x[:, 1]
        x = jnp.stack([real * c + imag * s, imag * c - real * s], axis=1)
        x = rotate_lanes(x.reshape(n * 2 * each * SUB, lanes), tables[1])
        x = rotate_sublanes(x.reshape(n * 2 * each, SUB, lanes), sc[1][1])
        x = x.reshape(n_bank, n_lane, 2, each, SUB, lanes)
        x = rotate_bits(x, n_bank, sc[1][2])
        x = jnp.stack([rotate_bits(x[b], n_lane, sc[1][3]) for b in range(n_bank)])
        turned[k] = x.reshape(n, 2, each, SUB, lanes)
        for device, there in peers:
            pltpu.make_async_remote_copy(
                src_ref=turned.at[k, there],
                dst_ref=back.at[k, me],
                send_sem=turn_sem.at[k],
                recv_sem=back_sem.at[k],
                device_id=device,
                device_id_type=MESH,
            ).start()
        back[k, me] = turned[k, me]

    high = tiles // units
    for k in range(chunks):
        wait_all(back.at[k], back_sem.at[k])
        x = back[k].reshape(blocks, high, 2, each, SUB, lanes)
        x = rotate_bits(x, blocks, sc[1][2])
        x = jnp.stack([rotate_bits(x[b], high, sc[1][1]) for b in range(blocks)])
        last[k] = x.reshape(n, 2, each, SUB, lanes)
    for part in range(2):
        for block in range(blocks):
            these = pl.ds(block * high, high)
            items = [last[u // each, these, part, u % each] for u in range(units)]
            x = jnp.stack(rotate_list(items, sc[1][1]), axis=1)
            out_ref[part, block] = x.reshape(rows, lanes)

    wait_all(level_recv, level_send_sem)
    for k in range(chunks):
        wait_all(recv.at[k], send_sem.at[k])
        wait_all(back.at[k], turn_sem.at[k])


def level_units(level, there, units):
    return level.at[pl.ds(there * units, units)]


def local(n_bank, n_lane, wave_parts, level_table, phase_angles, mix_angles):
    parts, blocks, rows, lanes = wave_parts.shape
    n = n_bank * n_lane
    tiles = rows // SUB
    units = blocks * tiles // n
    chunks = min(4, units)
    each = units // chunks
    operands = [
        wave_parts,
        level_table.reshape(blocks * tiles, SUB, lanes),
        phase_angles,
        mix_angles,
    ]
    exchange = pltpu.VMEM((chunks, n, 2, each, SUB, lanes), jnp.float32)
    dma = pltpu.SemaphoreType.DMA
    return pl.pallas_call(
        functools.partial(kernel, n_bank, n_lane, chunks),
        out_shape=jax.ShapeDtypeStruct(wave_parts.shape, jnp.float32),
        in_specs=[
            pl.BlockSpec(memory_space=pltpu.HBM),
            pl.BlockSpec(memory_space=pltpu.HBM),
            pl.BlockSpec(memory_space=pltpu.HBM),
            pl.BlockSpec(memory_space=pltpu.HBM),
        ],
        out_specs=pl.BlockSpec(memory_space=pltpu.VMEM),
        scratch_shapes=[
            pltpu.VMEM(wave_parts.shape, jnp.float32),
            pltpu.VMEM((blocks * tiles, SUB, lanes), jnp.float32),
            pltpu.VMEM(phase_angles.shape, jnp.float32),
            pltpu.SMEM(mix_angles.shape, jnp.float32),
            pltpu.VMEM((2, blocks, tiles, SUB, lanes), jnp.float32),
            exchange,
            exchange,
            pltpu.VMEM((n, units, SUB, lanes), jnp.float32),
            exchange,
            exchange,
            exchange,
            dma((4,)),
            dma,
            dma,
            dma((chunks,)),
            dma((chunks,)),
            dma((chunks,)),
            dma((chunks,)),
        ],
        compiler_params=pltpu.CompilerParams(
            collective_id=0, has_side_effects=True, vmem_limit_bytes=40 * 1024 * 1024
        ),
    )(*[pltpu.with_memory_space_constraint(value, pltpu.HBM) for value in operands])


def solution(mesh):
    placed = (
        P("site", ("bank", "lane"), None, None),
        P(("site", "bank", "lane"), None, None),
        P("site", None),
        P("site", None),
    )
    return jax.shard_map(
        functools.partial(local, mesh.shape["bank"], mesh.shape["lane"]),
        mesh=mesh,
        in_specs=placed,
        out_specs=P("site", ("bank", "lane"), None, None),
        check_vma=False,
    )
```

```python
import functools

import jax
import jax.numpy as jnp
from jax import lax
from jax.experimental import pallas as pl
from jax.experimental.pallas import tpu as pltpu
from jax.sharding import PartitionSpec as P

SUB = 8
MESH = pl.DeviceIdType.MESH


def sin_cos(turn):
    h = 0.5 * turn
    q = h * h
    s = -1.0 / 39916800 + q * (1.0 / 6227020800)
    for term in (1.0 / 362880, -1.0 / 5040, 1.0 / 120, -1.0 / 6, 1.0):
        s = term + q * s
    s = h * s
    c = -1.0 / 3628800 + q * (1.0 / 479001600)
    for term in (1.0 / 40320, -1.0 / 720, 1.0 / 24, -0.5, 1.0):
        c = term + q * c
    return 2.0 * s * c, 1.0 - 2.0 * s * s


def rotate_bits(x, count, sc):
    s, c = sc
    shape = x.shape
    step = 1
    while step < count:
        y = x.reshape(count // (2 * step), 2, step, *shape[1:])
        u, v = y[:, 0], y[:, 1]
        x = jnp.stack([c * u - s * v, c * v + s * u], axis=1).reshape(shape)
        step *= 2
    return x


def rotate_list(items, sc):
    s, c = sc
    step = 1
    while step < len(items):
        items = [
            c * x - s * items[i + step] if (i // step) % 2 == 0 else c * x + s * items[i - step]
            for i, x in enumerate(items)
        ]
        step *= 2
    return items


def differ(index, apart, count):
    out, bit = 0, 1
    while bit < count:
        out = out + lax.rem(index // bit + (apart // bit) % 2, 2) * bit
        bit *= 2
    return out


def rotate_sublanes(x, sc):
    s, c = sc
    place = lax.broadcasted_iota(jnp.int32, s.shape, 0)
    step = 1
    while step < SUB:
        upper = (place // step) % 2 == 1
        down = pltpu.roll(x, step, 1)
        if 2 * step == SUB:
            x = c * x + jnp.where(upper, s, -s) * down
        else:
            up = pltpu.roll(x, SUB - step, 1)
            x = c * x + jnp.where(upper, s, -s) * jnp.where(upper, down, up)
        step *= 2
    return x


def lane_table(sc, lanes):
    s = jnp.broadcast_to(sc[0][0:1], (lanes, lanes))
    c = jnp.broadcast_to(sc[1][0:1], (lanes, lanes))
    i = lax.broadcasted_iota(jnp.int32, (lanes, lanes), 0)
    j = lax.broadcasted_iota(jnp.int32, (lanes, lanes), 1)
    table = jnp.ones((lanes, lanes), jnp.float32)
    step = 1
    while step < lanes:
        a, b = (i // step) % 2, (j // step) % 2
        table = table * jnp.where(a == b, c, jnp.where(a > b, -s, s))
        step *= 2
    high = table.astype(jnp.bfloat16)
    low = (table - high.astype(jnp.float32)).astype(jnp.bfloat16)
    top = jnp.concatenate([high, low], axis=1)
    bottom = jnp.concatenate([high, jnp.zeros_like(low)], axis=1)
    return jnp.concatenate([top, bottom], axis=0)


def rotate_lanes(x, table):
    lanes = x.shape[1]
    high = x.astype(jnp.bfloat16)
    low = (x - high.astype(jnp.float32)).astype(jnp.bfloat16)
    out = jnp.dot(
        jnp.concatenate([high, low], axis=1), table, preferred_element_type=jnp.float32
    )
    return out[:, :lanes] + out[:, lanes:]


def kernel(
    n_bank, n_lane, chunks,
    wave_hbm, level_hbm, phase_hbm, mix_hbm, out_ref,
    wave, level, phase_ref, mix_ref, mixed, send, recv, level_recv, turned, back, last,
    in_sem, level_send_sem, level_recv_sem, send_sem, recv_sem, turn_sem, back_sem,
):
    n = n_bank * n_lane
    bank, lane = lax.axis_index("bank"), lax.axis_index("lane")
    me = bank * n_lane + lane
    _, blocks, rows, lanes = wave.shape
    tiles = rows // SUB
    units = blocks * tiles // n
    each = units // chunks

    peers = []
    for kb in range(n_bank):
        for kl in range(n_lane):
            if kb or kl:
                pb, pn = differ(bank, kb, n_bank), differ(lane, kl, n_lane)
                peers.append(({"bank": pb, "lane": pn}, pb * n_lane + pn))

    barrier = pltpu.get_barrier_semaphore()
    for device, _ in reversed(peers):
        pl.semaphore_signal(barrier, inc=1, device_id=device, device_id_type=MESH)
    loads = [
        pltpu.make_async_copy(there, here, in_sem.at[i])
        for i, (there, here) in enumerate(
            [(mix_hbm, mix_ref), (level_hbm, level), (phase_hbm, phase_ref), (wave_hbm, wave)]
        )
    ]
    for load in loads:
        load.start()

    loads[0].wait()
    sc = [[sin_cos(jnp.full((SUB, lanes), mix_ref[y, g], jnp.float32)) for g in range(4)] for y in range(2)]
    tables = [lane_table(sc[y][0], lanes) for y in range(2)]

    for load in loads[1:]:
        load.wait()
    pl.semaphore_wait(barrier, n - 1)
    for device, there in peers:
        pltpu.make_async_remote_copy(
            src_ref=level_units(level, there, units),
            dst_ref=level_recv.at[me],
            send_sem=level_send_sem,
            recv_sem=level_recv_sem,
            device_id=device,
            device_id_type=MESH,
        ).start()
    level_recv[me] = level_units(level, me, units)[...]

    for block in range(blocks):
        here = level[block * tiles : (block + 1) * tiles].reshape(rows, lanes)
        s, c = sin_cos(phase_ref[0:1, :] * here)
        real, imag = wave[0, block], wave[1, block]
        x = jnp.concatenate([real * c + imag * s, imag * c - real * s], axis=0)
        x = rotate_lanes(x, tables[0])
        x = rotate_sublanes(x.reshape(2 * tiles, SUB, lanes), sc[0][1])
        x = x.reshape(2, tiles, SUB, lanes)
        for part in range(2):
            mixed[part, block] = rotate_bits(x[part], tiles, sc[0][1])

    for part in range(2):
        x = rotate_bits(mixed[part], blocks, sc[0][2])
        x = x.reshape(n, chunks, each, SUB, lanes)
        for k in range(chunks):
            send[k, :, part] = x[:, k]
    for k in range(chunks):
        for device, there in peers:
            pltpu.make_async_remote_copy(
                src_ref=send.at[k, there],
                dst_ref=recv.at[k, me],
                send_sem=send_sem.at[k],
                recv_sem=recv_sem.at[k],
                device_id=device,
                device_id_type=MESH,
            ).start()
        recv[k, me] = send[k, me]

    def wait_all(buffer, sem):
        whole = buffer.at[pl.ds(0, n - 1)]
        pltpu.make_async_copy(whole, whole, sem).wait()

    wait_all(level_recv, level_recv_sem)
    for k in range(chunks):
        wait_all(recv.at[k], recv_sem.at[k])
        x = recv[k].reshape(n_bank, n_lane, 2, each, SUB, lanes)
        x = rotate_bits(x, n_bank, sc[0][2])
        x = jnp.stack([rotate_bits(x[b], n_lane, sc[0][3]) for b in range(n_bank)])
        x = x.reshape(n, 2, each, SUB, lanes)
        s, c = sin_cos(phase_ref[1:2, :] * level_recv[:, k * each : (k + 1) * each])
        real, imag = x[:, 0], x[:, 1]
        x = jnp.stack([real * c + imag * s, imag * c - real * s], axis=1)
        x = rotate_lanes(x.reshape(n * 2 * each * SUB, lanes), tables[1])
        x = rotate_sublanes(x.reshape(n * 2 * each, SUB, lanes), sc[1][1])
        x = x.reshape(n_bank, n_lane, 2, each, SUB, lanes)
        x = rotate_bits(x, n_bank, sc[1][2])
        x = jnp.stack([rotate_bits(x[b], n_lane, sc[1][3]) for b in range(n_bank)])
        turned[k] = x.reshape(n, 2, each, SUB, lanes)
        for device, there in peers:
            pltpu.make_async_remote_copy(
                src_ref=turned.at[k, there],
                dst_ref=back.at[k, me],
                send_sem=turn_sem.at[k],
                recv_sem=back_sem.at[k],
                device_id=device,
                device_id_type=MESH,
            ).start()
        back[k, me] = turned[k, me]

    high = tiles // units
    for k in range(chunks):
        wait_all(back.at[k], back_sem.at[k])
        x = back[k].reshape(blocks, high, 2, each, SUB, lanes)
        x = rotate_bits(x, blocks, sc[1][2])
        x = jnp.stack([rotate_bits(x[b], high, sc[1][1]) for b in range(blocks)])
        last[k] = x.reshape(n, 2, each, SUB, lanes)
    for part in range(2):
        for block in range(blocks):
            these = pl.ds(block * high, high)
            items = [last[u // each, these, part, u % each] for u in range(units)]
            x = jnp.stack(rotate_list(items, sc[1][1]), axis=1)
            out_ref[part, block] = x.reshape(rows, lanes)

    wait_all(level_recv, level_send_sem)
    for k in range(chunks):
        wait_all(recv.at[k], send_sem.at[k])
        wait_all(back.at[k], turn_sem.at[k])


def level_units(level, there, units):
    return level.at[pl.ds(there * units, units)]


def local(n_bank, n_lane, wave_parts, level_table, phase_angles, mix_angles):
    parts, blocks, rows, lanes = wave_parts.shape
    n = n_bank * n_lane
    tiles = rows // SUB
    units = blocks * tiles // n
    chunks = min(4, units)
    each = units // chunks
    operands = [
        wave_parts,
        level_table.reshape(blocks * tiles, SUB, lanes),
        phase_angles,
        mix_angles,
    ]
    exchange = pltpu.VMEM((chunks, n, 2, each, SUB, lanes), jnp.float32)
    dma = pltpu.SemaphoreType.DMA
    return pl.pallas_call(
        functools.partial(kernel, n_bank, n_lane, chunks),
        out_shape=jax.ShapeDtypeStruct(wave_parts.shape, jnp.float32),
        in_specs=[
            pl.BlockSpec(memory_space=pltpu.HBM),
            pl.BlockSpec(memory_space=pltpu.HBM),
            pl.BlockSpec(memory_space=pltpu.HBM),
            pl.BlockSpec(memory_space=pltpu.HBM),
        ],
        out_specs=pl.BlockSpec(memory_space=pltpu.VMEM),
        scratch_shapes=[
            pltpu.VMEM(wave_parts.shape, jnp.float32),
            pltpu.VMEM((blocks * tiles, SUB, lanes), jnp.float32),
            pltpu.VMEM(phase_angles.shape, jnp.float32),
            pltpu.SMEM(mix_angles.shape, jnp.float32),
            pltpu.VMEM((2, blocks, tiles, SUB, lanes), jnp.float32),
            exchange,
            exchange,
            pltpu.VMEM((n, units, SUB, lanes), jnp.float32),
            exchange,
            exchange,
            exchange,
            dma((4,)),
            dma,
            dma,
            dma((chunks,)),
            dma((chunks,)),
            dma((chunks,)),
            dma((chunks,)),
        ],
        compiler_params=pltpu.CompilerParams(
            collective_id=0, has_side_effects=True, vmem_limit_bytes=40 * 1024 * 1024
        ),
    )(*[pltpu.with_memory_space_constraint(value, pltpu.HBM) for value in operands])


def solution(mesh):
    placed = (
        P("site", ("bank", "lane"), None, None),
        P(("site", "bank", "lane"), None, None),
        P("site", None),
        P("site", None),
    )
    return jax.shard_map(
        functools.partial(local, mesh.shape["bank"], mesh.shape["lane"]),
        mesh=mesh,
        in_specs=placed,
        out_specs=P("site", ("bank", "lane"), None, None),
        check_vma=False,
    )
```
